32 devices in a mesh: dp: 2 (over x), t: 4 (over z), stage: 4 (over y, core).
Axes of the slice: x: 2, y: 2, z: 4, core: 2. Of those that a mesh axis runs over, the one named last changes fastest.
Arguments:
- hidden: bfloat16 [8, 8, 1536, 2048], P(('dp', 'stage')), parts along dimension 0
- w_query: bfloat16 [2048, 3072], P(None, 't')
- w_dkv: bfloat16 [2048, 576], replicated
- latent_gain: bfloat16 [512], replicated
- w_uk: bfloat16 [512, 2048], P(None, 't')
- w_uv: bfloat16 [512, 2048], P(None, 't')
- w_out: bfloat16 [2048, 2048], P('t')
Outputs:
- output 1: bfloat16 [8, 8, 1536, 2048], P(('dp', 'stage')), parts along dimension 0
- output 2: bfloat16 [8, 8, 1536, 576], P(('dp', 'stage'), 't'), parts along dimension 0
There are 2 independent parts. The reference program is written for one: setup_inputs(seed, part) draws one part's arguments, and reference() takes and returns one part's arrays. A program takes and returns all parts, laid end to end along the dimension named above; an argument that names none is the same for every part.
All inputs are finite; a program needn't handle non-finite values.
Results may differ from the reference program's by a relative error of at most 0.0108288.
Values are sent between devices in bfloat16 or wider.
A program may use at most 1 GiB of HBM per device.

```python
import jax
import jax.numpy as jnp
from jax import lax

D_MODEL = 2048
HEADS = 16
KV_RANK = 512
ROPE_DIM = 64
NOPE_DIM = 128
V_DIM = 128
STAGE_SLOTS = 4
REQUESTS = 8
SEQ_LEN = 1536

NORM_EPS = 1e-6
ROPE_BASE = 10000.0
HALF_ROPE = ROPE_DIM // 2
HEAD_DIM = NOPE_DIM + ROPE_DIM
PROMPT_SLOTS = STAGE_SLOTS // 2
N_BLOCKS = max(1, min(8, SEQ_LEN // 128))
BLOCK_LEN = SEQ_LEN // N_BLOCKS


def setup_inputs(seed: int = 0, part: int = 0) -> dict:
    part_key = jax.random.fold_in(jax.random.key(seed), part)
    shared = jax.random.split(jax.random.key(seed + 1), 6)
    hidden = jax.random.normal(part_key, (STAGE_SLOTS, REQUESTS, SEQ_LEN, D_MODEL), jnp.float32).astype(jnp.bfloat16)
    w_query = (jax.random.normal(shared[0], (D_MODEL, HEADS * HEAD_DIM), jnp.float32) * D_MODEL ** -0.5).astype(jnp.bfloat16)
    w_dkv = (jax.random.normal(shared[1], (D_MODEL, KV_RANK + ROPE_DIM), jnp.float32) * D_MODEL ** -0.5).astype(jnp.bfloat16)
    latent_gain = (1.0 + 0.3 * jax.random.normal(shared[2], (KV_RANK,), jnp.float32)).astype(jnp.bfloat16)
    w_uk = (jax.random.normal(shared[3], (KV_RANK, HEADS * NOPE_DIM), jnp.float32) * KV_RANK ** -0.5).astype(jnp.bfloat16)
    w_uv = (jax.random.normal(shared[4], (KV_RANK, HEADS * V_DIM), jnp.float32) * KV_RANK ** -0.5).astype(jnp.bfloat16)
    w_out = (jax.random.normal(shared[5], (HEADS * V_DIM, D_MODEL), jnp.float32) * (HEADS * V_DIM) ** -0.5).astype(jnp.bfloat16)
    return {"hidden": hidden, "w_query": w_query, "w_dkv": w_dkv, "latent_gain": latent_gain, "w_uk": w_uk, "w_uv": w_uv, "w_out": w_out}


def rope_tables():
    positions = jnp.arange(SEQ_LEN).astype(jnp.float32)
    inv_freq = ROPE_BASE ** (-jnp.arange(HALF_ROPE).astype(jnp.float32) / HALF_ROPE)
    angles = positions[:, None] * inv_freq[None, :]
    return jnp.cos(angles), jnp.sin(angles)


def apply_rope(vecs, cos_tab, sin_tab):
    as_f32 = vecs.astype(jnp.float32)
    low_half = as_f32[..., :HALF_ROPE]
    high_half = as_f32[..., HALF_ROPE:]
    rotated = jnp.concatenate([low_half * cos_tab - high_half * sin_tab, high_half * cos_tab + low_half * sin_tab], axis=-1)
    return rotated.astype(jnp.bfloat16)


def reference(hidden, w_query, w_dkv, latent_gain, w_uk, w_uv, w_out):
    cos_tab, sin_tab = rope_tables()

    def one_request(tokens):
        compressed = jnp.dot(tokens, w_dkv, preferred_element_type=jnp.float32).astype(jnp.bfloat16)
        c_raw = compressed[:, :KV_RANK].astype(jnp.float32)
        inv_rms = lax.rsqrt(jnp.mean(c_raw * c_raw, axis=-1, keepdims=True) + NORM_EPS)
        c_kv = (c_raw * inv_rms * latent_gain.astype(jnp.float32)).astype(jnp.bfloat16)
        k_rope = apply_rope(compressed[:, KV_RANK:], cos_tab, sin_tab)
        queries = jnp.dot(tokens, w_query, preferred_element_type=jnp.float32).astype(jnp.bfloat16)
        queries = queries.reshape(SEQ_LEN, HEADS, HEAD_DIM)
        q_nope = queries[:, :, :NOPE_DIM].astype(jnp.float32)
        q_rope = apply_rope(queries[:, :, NOPE_DIM:], cos_tab[:, None, :], sin_tab[:, None, :]).astype(jnp.float32)
        k_nope = jnp.dot(c_kv, w_uk, preferred_element_type=jnp.float32).astype(jnp.bfloat16)
        k_nope = k_nope.reshape(SEQ_LEN, HEADS, NOPE_DIM).astype(jnp.float32)
        values = jnp.dot(c_kv, w_uv, preferred_element_type=jnp.float32).astype(jnp.bfloat16)
        values = values.reshape(SEQ_LEN, HEADS, V_DIM).astype(jnp.float32)
        k_rope_f = k_rope.astype(jnp.float32)
        pieces = []
        for block_idx in range(N_BLOCKS):
            start_row = block_idx * BLOCK_LEN
            stop_row = start_row + BLOCK_LEN
            scores = jnp.einsum("qhe,khe->hqk", q_nope[start_row:stop_row], k_nope[:stop_row])
            scores = scores + jnp.einsum("qhe,ke->hqk", q_rope[start_row:stop_row], k_rope_f[:stop_row])
            q_pos = start_row + jnp.arange(BLOCK_LEN)[:, None]
            k_pos = jnp.arange(stop_row)[None, :]
            scores = jnp.where(k_pos <= q_pos, scores * HEAD_DIM ** -0.5, -jnp.inf)
            row_peak = jnp.max(scores, axis=-1, keepdims=True)
            weights = jnp.exp(scores - row_peak)
            row_total = jnp.sum(weights, axis=-1)
            mixed = jnp.einsum("hqk,khe->qhe", weights.astype(jnp.bfloat16).astype(jnp.float32), values[:stop_row])
            pieces.append((mixed / row_total.T[:, :, None]).astype(jnp.bfloat16))
        head_mix = jnp.concatenate(pieces, axis=0).reshape(SEQ_LEN, HEADS * V_DIM)
        out_rows = jnp.dot(head_mix, w_out, preferred_element_type=jnp.float32).astype(jnp.bfloat16)
        latent = jnp.concatenate([c_kv, k_rope], axis=-1)
        return out_rows, latent

    prompts = hidden[:PROMPT_SLOTS].reshape(PROMPT_SLOTS * REQUESTS, SEQ_LEN, D_MODEL)
    out_rows, latent = lax.map(one_request, prompts)
    out_rows = out_rows.reshape(PROMPT_SLOTS, REQUESTS, SEQ_LEN, D_MODEL)
    latent = latent.reshape(PROMPT_SLOTS, REQUESTS, SEQ_LEN, KV_RANK + ROPE_DIM)
    attn_out = jnp.concatenate([out_rows, jnp.zeros_like(out_rows)], axis=0)
    latent_cache = jnp.concatenate([jnp.zeros_like(latent), latent], axis=0)
    return attn_out, latent_cache
```

```python
import functools

import jax
import jax.numpy as jnp
from jax import lax
from jax.experimental import pallas as pl
from jax.experimental.pallas import tpu as pltpu
from jax.sharding import PartitionSpec as P


NOPE_DIM = 128
ROPE_DIM = 64
V_DIM = 128
HEAD_DIM = NOPE_DIM + ROPE_DIM
NORM_EPS = 1e-6
ROPE_BASE = 10000.0
LOG2E = 1.4426950408889634
ROWS = 512
Q_ROWS = 256


def rope_tables(seq_len):
    half_dim = ROPE_DIM // 2
    positions = jnp.arange(seq_len, dtype=jnp.float32)
    inv_freq = ROPE_BASE ** (-jnp.arange(half_dim, dtype=jnp.float32) / half_dim)
    angles = positions[:, None] * inv_freq[None, :]
    return jnp.cos(angles), jnp.sin(angles)


def swap_halves(w, is_low):
    return jnp.where(is_low, pltpu.roll(w, 96, 1), pltpu.roll(w, 32, 1))


def latent_kernel(kv_rank, merged, *refs):
    if merged:
        meta, x_ref, in_ref, wd_ref, gain_ref, cos_ref, sin_ref, xin_ref, ckv_ref, krp_ref = refs
    else:
        meta, x_ref, wd_ref, gain_ref, cos_ref, sin_ref, ckv_ref, krp_ref = refs
    f32 = jnp.float32

    def body():
        x = x_ref[0]
        if merged:
            x = jnp.where(meta[1] == 1, x, in_ref[0])
            xin_ref[0] = x
        comp = jnp.dot(x, wd_ref[...], preferred_element_type=f32).astype(jnp.bfloat16)
        raw = comp[:, :kv_rank].astype(f32)
        inv_rms = lax.rsqrt(jnp.mean(raw * raw, axis=-1, keepdims=True) + NORM_EPS)
        ckv_ref[0] = (raw * inv_rms * gain_ref[...]).astype(jnp.bfloat16)
        w = comp[:, kv_rank:].astype(f32)
        lane = lax.broadcasted_iota(jnp.int32, w.shape, 1)
        is_low = (lane % ROPE_DIM) < ROPE_DIM // 2
        roped = w * cos_ref[...] + swap_halves(w, is_low) * sin_ref[...]
        krp_ref[0, :, :128] = roped.astype(jnp.bfloat16)
        krp_ref[0, :, 128:] = pltpu.roll(roped, 64, 1).astype(jnp.bfloat16)

    pl.when(meta[0] == 1)(body)


def latent_call(meta, n_req, tokens, arrived, w_dkv, gain, cos, sin):
    _, seq_len, d_model = tokens.shape
    kv_rank = gain.shape[-1]
    in_specs = [pl.BlockSpec((1, ROWS, d_model), lambda r, i, m: (m[2 + r], i, 0))]
    operands = [meta, tokens]
    out_shape = [
        jax.ShapeDtypeStruct((n_req, seq_len, kv_rank), jnp.bfloat16),
        jax.ShapeDtypeStruct((n_req, seq_len, 256), jnp.bfloat16),
    ]
    out_specs = [
        pl.BlockSpec((1, ROWS, kv_rank), lambda r, i, m: (r, i, 0)),
        pl.BlockSpec((1, ROWS, 256), lambda r, i, m: (r, i, 0)),
    ]
    if arrived is not None:
        in_specs.append(pl.BlockSpec((1, ROWS, d_model), lambda r, i, m: (r, i, 0)))
        operands.append(arrived)
        out_shape.insert(0, jax.ShapeDtypeStruct((n_req, seq_len, d_model), jnp.bfloat16))
        out_specs.insert(0, pl.BlockSpec((1, ROWS, d_model), lambda r, i, m: (r, i, 0)))
    in_specs += [
        pl.BlockSpec(w_dkv.shape, lambda r, i, m: (0, 0)),
        pl.BlockSpec((1, kv_rank), lambda r, i, m: (0, 0)),
        pl.BlockSpec((ROWS, 128), lambda r, i, m: (i, 0)),
        pl.BlockSpec((ROWS, 128), lambda r, i, m: (i, 0)),
    ]
    return pl.pallas_call(
        functools.partial(latent_kernel, kv_rank, arrived is not None),
        out_shape=out_shape,
        grid_spec=pltpu.PrefetchScalarGridSpec(num_scalar_prefetch=1, grid=(n_req, seq_len // ROWS), in_specs=in_specs, out_specs=out_specs),
        compiler_params=pltpu.CompilerParams(vmem_limit_bytes=48 * 1024 * 1024),
        cost_estimate=pl.CostEstimate(flops=2 * n_req * seq_len * d_model * w_dkv.shape[1], bytes_accessed=n_req * seq_len * d_model * 2, transcendentals=0),
    )(*operands, w_dkv, gain, cos, sin)


def out_kernel(n_cols, *refs):
    meta, o_ref, w_ref = refs[:3]
    y_ref = refs[-1]

    def multiply(n, carry):
        cols = pl.ds(pl.multiple_of(n * ROWS, ROWS), ROWS)
        y_ref[0, :, cols] = jnp.dot(o_ref[0], w_ref[:, cols], preferred_element_type=jnp.float32).astype(jnp.bfloat16)
        return carry

    @pl.when(meta[0] == 1)
    def _():
        lax.fori_loop(0, n_cols // ROWS, multiply, 0)

    @pl.when(meta[0] != 1)
    def _():
        y_ref[...] = jnp.zeros_like(y_ref)


def out_call(meta, n_req, first_req, o_mix, w_out, into):
    _, seq_len, depth = o_mix.shape
    d_model = w_out.shape[1]
    block = (1, ROWS, d_model)
    in_specs = [pl.BlockSpec((1, ROWS, depth), lambda r, i, m: (r + first_req, i, 0)), pl.BlockSpec(w_out.shape, lambda r, i, m: (0, 0))]
    operands = [meta, o_mix, w_out]
    aliases = {}
    out_shape = jax.ShapeDtypeStruct((n_req, seq_len, d_model), jnp.bfloat16)
    if into is not None:
        in_specs.append(pl.BlockSpec(memory_space=pl.ANY))
        operands.append(into)
        aliases = {3: 0}
        out_shape = jax.ShapeDtypeStruct(into.shape, jnp.bfloat16)
    return pl.pallas_call(
        functools.partial(out_kernel, d_model),
        out_shape=out_shape,
        grid_spec=pltpu.PrefetchScalarGridSpec(num_scalar_prefetch=1, grid=(n_req, seq_len // ROWS), in_specs=in_specs, out_specs=pl.BlockSpec(block, lambda r, i, m: (m[1 + r], i, 0))),
        input_output_aliases=aliases,
        compiler_params=pltpu.CompilerParams(vmem_limit_bytes=48 * 1024 * 1024),
        cost_estimate=pl.CostEstimate(flops=2 * n_req * seq_len * depth * d_model, bytes_accessed=n_req * seq_len * d_model * 4, transcendentals=0),
    )(*operands)


def heads_kernel(n_heads, seq_len, chained, *refs):
    if chained:
        meta, x_ref, ckv_ref, krp_ref, wq_ref, wukv_ref, cos_ref, sin_ref, _, o_ref, q_s, k_s, v_s = refs
    else:
        meta, x_ref, ckv_ref, krp_ref, wq_ref, wukv_ref, cos_ref, sin_ref, o_ref, q_s, k_s, v_s = refs
    nope_cols = n_heads * NOPE_DIM
    f32 = jnp.float32

    def project(block_idx, carry):
        rows = pl.ds(pl.multiple_of(block_idx * ROWS, ROWS), ROWS)
        lat = ckv_ref[0, rows, :]
        k_nope = jnp.dot(lat, wukv_ref[0, :, :nope_cols], preferred_element_type=f32).astype(jnp.bfloat16)
        v_s[rows, :] = jnp.dot(lat, wukv_ref[0, :, nope_cols:], preferred_element_type=f32).astype(jnp.bfloat16)
        x = x_ref[0, rows, :]
        q_nope = jnp.dot(x, wq_ref[0, :, :nope_cols], preferred_element_type=f32).astype(jnp.bfloat16)
        q_rope = jnp.dot(x, wq_ref[0, :, nope_cols:], preferred_element_type=f32).astype(jnp.bfloat16)
        cos, sin = cos_ref[rows, :], sin_ref[rows, :]
        lane = lax.broadcasted_iota(jnp.int32, (ROWS, 128), 1)
        is_low = (lane % ROPE_DIM) < ROPE_DIM // 2
        for h in range(n_heads):
            if h % 2 == 0:
                w = q_rope[:, h * ROPE_DIM : h * ROPE_DIM + 128].astype(f32)
                roped = (w * cos + swap_halves(w, is_low) * sin).astype(jnp.bfloat16)
            q_s[h, rows, :NOPE_DIM] = q_nope[:, h * NOPE_DIM : (h + 1) * NOPE_DIM]
            q_s[h, rows, NOPE_DIM:] = roped
            k_s[h, rows, :NOPE_DIM] = k_nope[:, h * NOPE_DIM : (h + 1) * NOPE_DIM]
            k_s[h, rows, NOPE_DIM:] = krp_ref[0, rows, (h % 2) * 128 : (h % 2 + 1) * 128]
        return carry

    exponent_scale = HEAD_DIM ** -0.5 * LOG2E
    row = lax.broadcasted_iota(jnp.int32, (Q_ROWS, Q_ROWS), 0)
    col = lax.broadcasted_iota(jnp.int32, (Q_ROWS, Q_ROWS), 1)
    nt = (((1,), (1,)), ((), ()))

    n_blocks = seq_len // Q_ROWS

    def score(h, block_idx):
        start = block_idx * Q_ROWS
        q = q_s[h, start : start + Q_ROWS, :]
        s_diag = lax.dot_general(q, k_s[h, start : start + Q_ROWS, :], nt, preferred_element_type=f32)
        s_diag = jnp.where(col <= row, s_diag, -jnp.inf)
        if block_idx == 0:
            return (s_diag,)
        return s_diag, lax.dot_general(q, k_s[h, :start, :], nt, preferred_element_type=f32)

    def weigh(scores):
        peak = functools.reduce(jnp.maximum, [jnp.max(s, axis=-1, keepdims=True) for s in scores])
        weights = [jnp.exp2((s - peak) * exponent_scale) for s in scores]
        total = functools.reduce(jnp.add, [jnp.sum(e, axis=-1, keepdims=True) for e in weights])
        return [e.astype(jnp.bfloat16) for e in weights], total

    def mix(h, block_idx, weights, total):
        start = block_idx * Q_ROWS
        cols = pl.ds(pl.multiple_of(h * V_DIM, V_DIM), V_DIM)
        mixed = jnp.dot(weights[0], v_s[start : start + Q_ROWS, cols], preferred_element_type=f32)
        if block_idx:
            mixed = mixed + jnp.dot(weights[1], v_s[:start, cols], preferred_element_type=f32)
        o_ref[0, start : start + Q_ROWS, cols] = (mixed / total).astype(jnp.bfloat16)

    def attend(h, carry):
        tasks = [(h, block_idx) for block_idx in (*range(1, n_blocks, 2), *range((n_blocks - 1) // 2 * 2, -1, -2))]
        scores = {0: score(*tasks[0])}
        weights = {}
        for i in range(len(tasks)):
            if i + 1 < len(tasks):
                scores[i + 1] = score(*tasks[i + 1])
            if i:
                mix(*tasks[i - 1], *weights.pop(i - 1))
            weights[i] = weigh(scores.pop(i))
            if i + 1 == len(tasks):
                mix(*tasks[i], *weights.pop(i))

        return carry

    @pl.when(meta[0] == 1)
    def _():
        lax.fori_loop(0, seq_len // ROWS, project, 0)
        lax.fori_loop(0, n_heads, attend, 0)


def heads_call(meta, n_shards, n_req, first_req, tokens, c_kv, krp, wq, wukv, cos, sin, o_total, o_in):
    _, seq_len, d_model = tokens.shape
    kv_rank = c_kv.shape[-1]
    n_heads = wukv.shape[-1] // (NOPE_DIM + V_DIM)
    q_cols = wq.shape[-1]
    where_x = 1 + 2 * n_shards
    in_specs = [
        pl.BlockSpec((1, seq_len, d_model), lambda j, r, m: (m[where_x + r], 0, 0)),
        pl.BlockSpec((1, seq_len, kv_rank), lambda j, r, m: (r + first_req, 0, 0)),
        pl.BlockSpec((1, seq_len, 256), lambda j, r, m: (r + first_req, 0, 0)),
        pl.BlockSpec((1, d_model, q_cols), lambda j, r, m: (m[1 + j], 0, 0)),
        pl.BlockSpec((1, kv_rank, wukv.shape[-1]), lambda j, r, m: (m[1 + j], 0, 0)),
        pl.BlockSpec((seq_len, 128), lambda j, r, m: (0, 0)),
        pl.BlockSpec((seq_len, 128), lambda j, r, m: (0, 0)),
    ]
    operands = [meta, tokens, c_kv, krp, wq, wukv, cos, sin]
    aliases = {}
    out_shape = jax.ShapeDtypeStruct((c_kv.shape[0], seq_len, o_total), jnp.bfloat16)
    if o_in is not None:
        in_specs.append(pl.BlockSpec(memory_space=pl.ANY))
        operands.append(o_in)
        aliases = {8: 0}
    rows = n_shards * n_req * seq_len
    flops = 2 * rows * (d_model * q_cols + kv_rank * wukv.shape[-1] + n_heads * (seq_len // 2 + 128) * 512)
    return pl.pallas_call(
        functools.partial(heads_kernel, n_heads, seq_len, o_in is not None),
        out_shape=out_shape,
        grid_spec=pltpu.PrefetchScalarGridSpec(
            num_scalar_prefetch=1,
            grid=(n_shards, n_req),
            in_specs=in_specs,
            out_specs=pl.BlockSpec((1, seq_len, n_heads * V_DIM), lambda j, r, m: (r + first_req, 0, m[1 + n_shards + j])),
            scratch_shapes=[
                pltpu.VMEM((n_heads, seq_len, 256), jnp.bfloat16),
                pltpu.VMEM((n_heads, seq_len, 256), jnp.bfloat16),
                pltpu.VMEM((seq_len, n_heads * V_DIM), jnp.bfloat16),
            ],
        ),
        input_output_aliases=aliases,
        compiler_params=pltpu.CompilerParams(vmem_limit_bytes=60 * 1024 * 1024),
        cost_estimate=pl.CostEstimate(flops=flops, bytes_accessed=rows * d_model * 2, transcendentals=0),
    )(*operands)


def solution(mesh):
    n_tp = mesh.shape["t"]
    n_stage = mesh.shape["stage"]
    half_stage = n_stage // 2
    hand_pairs = [(s, s + half_stage) for s in range(half_stage)]
    back_pairs = [(s + half_stage, s) for s in range(half_stage)]
    twin_pairs = [(s, s ^ 1) for s in range(n_stage)]
    slot_spec = P(("dp", "stage"), None, None, None)
    cache_spec = P(("dp", "stage"), "t", None, None)

    def gather_shards(w_local):
        is_second = lax.axis_index("stage") % 2
        half = w_local.shape[0] // 2
        mine = lax.dynamic_slice_in_dim(w_local, is_second * half, half, axis=0)
        mine_all = lax.all_gather(mine, "t", axis=0, tiled=False)
        twin_all = lax.ppermute(mine_all, "stage", twin_pairs)
        low = jnp.where(is_second == 0, mine_all, twin_all)
        high = jnp.where(is_second == 0, twin_all, mine_all)
        return jnp.concatenate([low, high], axis=1)

    def layer(hidden, w_query, w_dkv, latent_gain, w_uk, w_uv, w_out):
        tokens = hidden[0]
        batch, seq_len, d_model = tokens.shape
        t_index = lax.axis_index("t")
        is_prompt = (lax.axis_index("stage") < half_stage).astype(jnp.int32)
        cos_tab, sin_tab = rope_tables(seq_len)
        cos4 = jnp.concatenate([cos_tab] * 4, axis=-1)
        sin4 = jnp.concatenate([-sin_tab, sin_tab, -sin_tab, sin_tab], axis=-1)

        n_away = batch // n_tp
        n_main = 3
        x_a = lax.ppermute(lax.dynamic_slice_in_dim(tokens, t_index * n_away, 1, axis=0), "stage", hand_pairs)
        x_b = lax.ppermute(lax.dynamic_slice_in_dim(tokens, t_index * n_away + 1, 1, axis=0), "stage", hand_pairs)

        n_heads = w_uk.shape[1] // NOPE_DIM
        by_head = w_query.reshape(d_model, n_heads, HEAD_DIM)
        wq_local = jnp.concatenate([by_head[:, :, :NOPE_DIM].reshape(d_model, -1), by_head[:, :, NOPE_DIM:].reshape(d_model, -1)], axis=1)
        wukv_local = jnp.concatenate([w_uk, w_uv], axis=1)
        wq_all = gather_shards(wq_local)
        wukv_all = gather_shards(wukv_local)
        wo_all = gather_shards(w_out)
        o_total = n_tp * n_heads * V_DIM
        wo_all = wo_all.reshape(o_total, d_model)

        odd = lax.rem(t_index, 2)
        neighbour = t_index + 1 - 2 * odd
        common = 2 * n_away * (1 - t_index // 2)
        order = jnp.stack([common + n_away + odd, common, common + 1, neighbour * n_away, neighbour * n_away + 1]).astype(jnp.int32)
        swapped_in = common + n_away + 1 - odd
        wd = jnp.concatenate([w_dkv, jnp.zeros((d_model, 128 - ROPE_DIM), w_dkv.dtype)], axis=1)
        gain = latent_gain.astype(jnp.float32)[None]
        one = jnp.ones((1,), jnp.int32)
        zero = jnp.zeros((1,), jnp.int32)
        prompt = is_prompt[None]
        here = t_index[None].astype(jnp.int32)
        away = lax.rem(t_index + 1 + jnp.arange(n_tp - 1, dtype=jnp.int32), n_tp)
        order_here = order * is_prompt
        tables = (cos4, sin4)

        def meta(*parts):
            return jnp.concatenate([p.astype(jnp.int32) for p in parts])

        def local_heads(active, xs, n_req, first, x, ckv, krp):
            return heads_call(meta(active, zero, here, xs), 1, n_req, first, x, ckv, krp, wq_local[None], wukv_local[None], *tables, o_total, None)

        def rest_heads(active, xs, n_req, first, x, ckv, krp, o_mix):
            return heads_call(meta(active, away, away, xs), n_tp - 1, n_req, first, x, ckv, krp, wq_all, wukv_all, *tables, o_total, o_mix)

        ckv, krp = latent_call(meta(prompt, prompt, order_here[:n_main]), n_main, tokens, None, wd, gain, *tables)
        o_swap = local_heads(prompt, order_here[:1], 1, 0, tokens, ckv, krp)
        o_main = local_heads(prompt, order_here[1:n_main], n_main - 1, 1, tokens, ckv, krp)

        def shared(slot, arrived):
            x, ckv_s, krp_s = latent_call(meta(one, prompt, order_here[slot : slot + 1]), 1, tokens, arrived, wd, gain, *tables)
            o_s = local_heads(one, zero, 1, 0, x, ckv_s, krp_s)
            o_s = rest_heads(one, zero, 1, 0, x, ckv_s, krp_s, o_s)
            y_s = out_call(meta(one, zero), 1, 0, o_s, wo_all, None)
            back = lax.ppermute(y_s, "stage", back_pairs)
            return y_s, back, jnp.concatenate([ckv_s, krp_s[..., :ROPE_DIM]], axis=-1)

        y_a, back_a, latent_a = shared(n_main, x_a)
        o_swap = rest_heads(prompt, order_here[:1], 1, 0, tokens, ckv, krp, o_swap)
        y_swap = out_call(meta(prompt, zero), 1, 0, o_swap, wo_all, None)
        from_neighbour = lax.ppermute(y_swap, "t", [(t, t ^ 1) for t in range(n_tp)])
        y_b, back_b, latent_b = shared(n_main + 1, x_b)
        o_main = rest_heads(prompt, order_here[1:n_main], n_main - 1, 1, tokens, ckv, krp, o_main)

        rows = jnp.zeros((batch, seq_len, d_model), jnp.bfloat16)
        rows = out_call(meta(prompt, order[1:n_main]), n_main - 1, 1, o_main, wo_all, rows)
        for y_s, slot in ((y_a, n_main), (y_b, n_main + 1), (y_swap, 0)):
            rows = lax.dynamic_update_slice_in_dim(rows, jnp.where(is_prompt == 1, y_s, jnp.zeros_like(y_s)), order[slot], axis=0)
        for back, place in ((back_a, t_index * n_away), (from_neighbour, swapped_in), (back_b, t_index * n_away + 1)):
            rows = lax.dynamic_update_slice_in_dim(rows, back, place, axis=0)
        latent = jnp.concatenate([latent_a, latent_b], axis=0)
        latent = jnp.where(is_prompt == 1, jnp.zeros_like(latent), latent)
        return rows[None], latent[None]

    return jax.shard_map(layer, mesh=mesh, in_specs=(slot_spec, P(None, "t"), P(None, None), P(None), P(None, "t"), P(None, "t"), P("t", None)), out_specs=(slot_spec, cache_spec), check_vma=False)
```

```python
import functools

import jax
import jax.numpy as jnp
from jax import lax
from jax.experimental import pallas as pl
from jax.experimental.pallas import tpu as pltpu
from jax.sharding import PartitionSpec as P


NOPE_DIM = 128
ROPE_DIM = 64
V_DIM = 128
HEAD_DIM = NOPE_DIM + ROPE_DIM
NORM_EPS = 1e-6
ROPE_BASE = 10000.0
LOG2E = 1.4426950408889634
ROWS = 512
Q_ROWS = 256


def rope_tables(seq_len):
    half_dim = ROPE_DIM // 2
    positions = jnp.arange(seq_len, dtype=jnp.float32)
    inv_freq = ROPE_BASE ** (-jnp.arange(half_dim, dtype=jnp.float32) / half_dim)
    angles = positions[:, None] * inv_freq[None, :]
    return jnp.cos(angles), jnp.sin(angles)


def swap_halves(w, is_low):
    return jnp.where(is_low, pltpu.roll(w, 96, 1), pltpu.roll(w, 32, 1))


def latent_kernel(kv_rank, meta, x_ref, wd_ref, gain_ref, cos_ref, sin_ref, ckv_ref, krp_ref):
    f32 = jnp.float32

    def body():
        comp = jnp.dot(x_ref[0], wd_ref[...], preferred_element_type=f32).astype(jnp.bfloat16)
        raw = comp[:, :kv_rank].astype(f32)
        inv_rms = lax.rsqrt(jnp.mean(raw * raw, axis=-1, keepdims=True) + NORM_EPS)
        ckv_ref[0] = (raw * inv_rms * gain_ref[...]).astype(jnp.bfloat16)
        w = comp[:, kv_rank:].astype(f32)
        lane = lax.broadcasted_iota(jnp.int32, w.shape, 1)
        is_low = (lane % ROPE_DIM) < ROPE_DIM // 2
        roped = w * cos_ref[...] + swap_halves(w, is_low) * sin_ref[...]
        krp_ref[0, :, :128] = roped.astype(jnp.bfloat16)
        krp_ref[0, :, 128:] = pltpu.roll(roped, 64, 1).astype(jnp.bfloat16)

    pl.when(meta[0] == 1)(body)


def latent_call(meta, n_req, tokens, w_dkv, gain, cos, sin):
    _, seq_len, d_model = tokens.shape
    kv_rank = gain.shape[-1]
    in_specs = [pl.BlockSpec((1, ROWS, d_model), lambda r, i, m: (m[1 + r], i * m[0], 0))]
    operands = [meta, tokens]
    out_shape = [
        jax.ShapeDtypeStruct((n_req, seq_len, kv_rank), jnp.bfloat16),
        jax.ShapeDtypeStruct((n_req, seq_len, 256), jnp.bfloat16),
    ]
    out_specs = [
        pl.BlockSpec((1, ROWS, kv_rank), lambda r, i, m: (r * m[0], i * m[0], 0)),
        pl.BlockSpec((1, ROWS, 256), lambda r, i, m: (r * m[0], i * m[0], 0)),
    ]
    in_specs += [
        pl.BlockSpec(w_dkv.shape, lambda r, i, m: (0, 0)),
        pl.BlockSpec((1, kv_rank), lambda r, i, m: (0, 0)),
        pl.BlockSpec((ROWS, 128), lambda r, i, m: (i, 0)),
        pl.BlockSpec((ROWS, 128), lambda r, i, m: (i, 0)),
    ]
    return pl.pallas_call(
        functools.partial(latent_kernel, kv_rank),
        out_shape=out_shape,
        grid_spec=pltpu.PrefetchScalarGridSpec(num_scalar_prefetch=1, grid=(n_req, seq_len // ROWS), in_specs=in_specs, out_specs=out_specs),
        compiler_params=pltpu.CompilerParams(vmem_limit_bytes=48 * 1024 * 1024),
        cost_estimate=pl.CostEstimate(flops=2 * n_req * seq_len * d_model * w_dkv.shape[1], bytes_accessed=n_req * seq_len * d_model * 2, transcendentals=0),
    )(*operands, w_dkv, gain, cos, sin)


def out_kernel(n_cols, meta, o_ref, mine_ref, twin_ref, *refs):
    y_ref, w_ref = refs[-2:]
    n_shards, half, _ = mine_ref.shape

    @pl.when(meta[0] * (pl.program_id(0) == 0) * (pl.program_id(1) == 0) == 1)
    def _():
        for j in range(n_shards):
            for part_ref, second in ((mine_ref, meta[1]), (twin_ref, 1 - meta[1])):
                w_ref[pl.ds(pl.multiple_of((2 * j + second) * half, half), half), :] = part_ref[j]

    def multiply(n, carry):
        cols = pl.ds(pl.multiple_of(n * ROWS, ROWS), ROWS)
        y_ref[0, :, cols] = jnp.dot(o_ref[0], w_ref[:, cols], preferred_element_type=jnp.float32).astype(jnp.bfloat16)
        return carry

    @pl.when(meta[0] == 1)
    def _():
        lax.fori_loop(0, n_cols // ROWS, multiply, 0)

    @pl.when(meta[0] != 1)
    def _():
        y_ref[...] = jnp.zeros_like(y_ref)


def out_call(meta, n_req, first_req, o_mix, w_mine, w_twin, n_rows, idle_rows):
    _, seq_len, depth = o_mix.shape
    d_model = w_mine.shape[-1]
    in_specs = [
        pl.BlockSpec((1, ROWS, depth), lambda r, i, m: ((r + first_req) * m[0], i * m[0], 0)),
        pl.BlockSpec(w_mine.shape, lambda r, i, m: (0, 0, 0)),
        pl.BlockSpec(w_twin.shape, lambda r, i, m: (0, 0, 0)),
    ]
    operands = [meta, o_mix, w_mine, w_twin]
    block = (1, ROWS, d_model)
    return pl.pallas_call(
        functools.partial(out_kernel, d_model),
        out_shape=jax.ShapeDtypeStruct((n_rows, seq_len, d_model), jnp.bfloat16),
        grid_spec=pltpu.PrefetchScalarGridSpec(num_scalar_prefetch=1, grid=(n_req, seq_len // ROWS), in_specs=in_specs, out_specs=pl.BlockSpec(block, lambda r, i, m: (m[2 + r], i if idle_rows else i * m[0], 0)), scratch_shapes=[pltpu.VMEM((depth, d_model), jnp.bfloat16)]),
        compiler_params=pltpu.CompilerParams(vmem_limit_bytes=48 * 1024 * 1024),
        cost_estimate=pl.CostEstimate(flops=2 * n_req * seq_len * depth * d_model, bytes_accessed=n_req * seq_len * d_model * 4, transcendentals=0),
    )(*operands)


def heads_kernel(n_heads, seq_len, chained, *refs):
    if chained:
        meta, x_ref, ckv_ref, krp_ref, mine_ref, twin_ref, wukv_ref, cos_ref, sin_ref, _, o_ref, q_s, k_s, v_s, wq_s = refs
    else:
        meta, x_ref, ckv_ref, krp_ref, mine_ref, twin_ref, wukv_ref, cos_ref, sin_ref, o_ref, q_s, k_s, v_s, wq_s = refs
    nope_cols = n_heads * NOPE_DIM
    f32 = jnp.float32

    def project(block_idx, carry):
        rows = pl.ds(pl.multiple_of(block_idx * ROWS, ROWS), ROWS)
        lat = ckv_ref[0, rows, :]
        k_nope = jnp.dot(lat, wukv_ref[0, :, :nope_cols], preferred_element_type=f32).astype(jnp.bfloat16)
        v_s[rows, :] = jnp.dot(lat, wukv_ref[0, :, nope_cols:], preferred_element_type=f32).astype(jnp.bfloat16)
        x = x_ref[0, rows, :]
        q_nope = jnp.dot(x, wq_s[:, :nope_cols], preferred_element_type=f32).astype(jnp.bfloat16)
        q_rope = jnp.dot(x, wq_s[:, nope_cols:], preferred_element_type=f32).astype(jnp.bfloat16)
        cos, sin = cos_ref[rows, :], sin_ref[rows, :]
        lane = lax.broadcasted_iota(jnp.int32, (ROWS, 128), 1)
        is_low = (lane % ROPE_DIM) < ROPE_DIM // 2
        for h in range(n_heads):
            if h % 2 == 0:
                w = q_rope[:, h * ROPE_DIM : h * ROPE_DIM + 128].astype(f32)
                roped = (w * cos + swap_halves(w, is_low) * sin).astype(jnp.bfloat16)
            q_s[h, rows, :NOPE_DIM] = q_nope[:, h * NOPE_DIM : (h + 1) * NOPE_DIM]
            q_s[h, rows, NOPE_DIM:] = roped
            k_s[h, rows, :NOPE_DIM] = k_nope[:, h * NOPE_DIM : (h + 1) * NOPE_DIM]
            k_s[h, rows, NOPE_DIM:] = krp_ref[0, rows, (h % 2) * 128 : (h % 2 + 1) * 128]
        return carry

    exponent_scale = HEAD_DIM ** -0.5 * LOG2E
    row = lax.broadcasted_iota(jnp.int32, (Q_ROWS, Q_ROWS), 0)
    col = lax.broadcasted_iota(jnp.int32, (Q_ROWS, Q_ROWS), 1)
    nt = (((1,), (1,)), ((), ()))

    n_blocks = seq_len // Q_ROWS

    def score(h, block_idx):
        start = block_idx * Q_ROWS
        q = q_s[h, start : start + Q_ROWS, :]
        s_diag = lax.dot_general(q, k_s[h, start : start + Q_ROWS, :], nt, preferred_element_type=f32)
        s_diag = jnp.where(col <= row, s_diag, -jnp.inf)
        if block_idx == 0:
            return (s_diag,)
        return s_diag, lax.dot_general(q, k_s[h, :start, :], nt, preferred_element_type=f32)

    def weigh(scores):
        peak = functools.reduce(jnp.maximum, [jnp.max(s, axis=-1, keepdims=True) for s in scores])
        weights = [jnp.exp2((s - peak) * exponent_scale) for s in scores]
        total = functools.reduce(jnp.add, [jnp.sum(e, axis=-1, keepdims=True) for e in weights])
        return [e.astype(jnp.bfloat16) for e in weights], total

    def mix(h, block_idx, weights, total):
        start = block_idx * Q_ROWS
        cols = pl.ds(pl.multiple_of(h * V_DIM, V_DIM), V_DIM)
        mixed = jnp.dot(weights[0], v_s[start : start + Q_ROWS, cols], preferred_element_type=f32)
        if block_idx:
            mixed = mixed + jnp.dot(weights[1], v_s[:start, cols], preferred_element_type=f32)
        o_ref[0, start : start + Q_ROWS, cols] = (mixed / total).astype(jnp.bfloat16)

    def attend(h, carry):
        tasks = [(h, block_idx) for block_idx in (*range(1, n_blocks, 2), *range((n_blocks - 1) // 2 * 2, -1, -2))]
        scores = {0: score(*tasks[0])}
        weights = {}
        for i in range(len(tasks)):
            if i + 1 < len(tasks):
                scores[i + 1] = score(*tasks[i + 1])
            if i:
                mix(*tasks[i - 1], *weights.pop(i - 1))
            weights[i] = weigh(scores.pop(i))
            if i + 1 == len(tasks):
                mix(*tasks[i], *weights.pop(i))

        return carry

    half = mine_ref.shape[1]

    @pl.when(meta[0] * (pl.program_id(1) == 0) == 1)
    def _():
        wq_s[pl.ds(pl.multiple_of(meta[1] * half, half), half), :] = mine_ref[0]
        wq_s[pl.ds(pl.multiple_of((1 - meta[1]) * half, half), half), :] = twin_ref[0]

    @pl.when(meta[0] == 1)
    def _():
        lax.fori_loop(0, seq_len // ROWS, project, 0)
        lax.fori_loop(0, n_heads, attend, 0)


def heads_call(meta, n_shards, n_req, first_req, tokens, c_kv, krp, wq_mine, wq_twin, twin_block, wukv, cos, sin, o_total, o_in):
    _, seq_len, d_model = tokens.shape
    kv_rank = c_kv.shape[-1]
    n_heads = wukv.shape[-1] // (NOPE_DIM + V_DIM)
    q_cols = wq_mine.shape[-1]
    where_x = 2 + 2 * n_shards
    in_specs = [
        pl.BlockSpec((1, seq_len, d_model), lambda j, r, m: (m[where_x + r], 0, 0)),
        pl.BlockSpec((1, seq_len, kv_rank), lambda j, r, m: ((r + first_req) * m[0], 0, 0)),
        pl.BlockSpec((1, seq_len, 256), lambda j, r, m: ((r + first_req) * m[0], 0, 0)),
        pl.BlockSpec((1, d_model // 2, q_cols), lambda j, r, m: (m[2 + j], 0, 0)),
        pl.BlockSpec((1, d_model // 2, q_cols), lambda j, r, m: (m[2 + j], twin_block, 0)),
        pl.BlockSpec((1, kv_rank, wukv.shape[-1]), lambda j, r, m: (m[2 + j], 0, 0)),
        pl.BlockSpec((seq_len, 128), lambda j, r, m: (0, 0)),
        pl.BlockSpec((seq_len, 128), lambda j, r, m: (0, 0)),
    ]
    operands = [meta, tokens, c_kv, krp, wq_mine, wq_twin, wukv, cos, sin]
    aliases = {}
    out_shape = jax.ShapeDtypeStruct((c_kv.shape[0], seq_len, o_total), jnp.bfloat16)
    if o_in is not None:
        in_specs.append(pl.BlockSpec(memory_space=pl.ANY))
        operands.append(o_in)
        aliases = {9: 0}
    rows = n_shards * n_req * seq_len
    flops = 2 * rows * (d_model * q_cols + kv_rank * wukv.shape[-1] + n_heads * (seq_len // 2 + 128) * 512)
    return pl.pallas_call(
        functools.partial(heads_kernel, n_heads, seq_len, o_in is not None),
        out_shape=out_shape,
        grid_spec=pltpu.PrefetchScalarGridSpec(
            num_scalar_prefetch=1,
            grid=(n_shards, n_req),
            in_specs=in_specs,
            out_specs=pl.BlockSpec((1, seq_len, n_heads * V_DIM), lambda j, r, m: ((r + first_req) * m[0], 0, m[2 + n_shards + j])),
            scratch_shapes=[
                pltpu.VMEM((n_heads, seq_len, 256), jnp.bfloat16),
                pltpu.VMEM((n_heads, seq_len, 256), jnp.bfloat16),
                pltpu.VMEM((seq_len, n_heads * V_DIM), jnp.bfloat16),
                pltpu.VMEM((d_model, q_cols), jnp.bfloat16),
            ],
        ),
        input_output_aliases=aliases,
        compiler_params=pltpu.CompilerParams(vmem_limit_bytes=60 * 1024 * 1024),
        cost_estimate=pl.CostEstimate(flops=flops, bytes_accessed=rows * d_model * 2, transcendentals=0),
    )(*operands)


def solution(mesh):
    n_tp = mesh.shape["t"]
    n_stage = mesh.shape["stage"]
    half_stage = n_stage // 2
    hand_pairs = [(s, s + half_stage) for s in range(half_stage)]
    back_pairs = [(s + half_stage, s) for s in range(half_stage)]
    twin_pairs = [(s, s ^ 1) for s in range(n_stage)]
    slot_spec = P(("dp", "stage"), None, None, None)
    cache_spec = P(("dp", "stage"), "t", None, None)

    def gather_shards(w_local):
        is_second = lax.axis_index("stage") % 2
        half = w_local.shape[0] // 2
        mine = lax.dynamic_slice_in_dim(w_local, is_second * half, half, axis=0)
        mine_all = lax.all_gather(mine, "t", axis=0, tiled=False)
        twin_all = lax.ppermute(mine_all, "stage", twin_pairs)
        return mine_all, twin_all

    def join_halves(mine_all, twin_all):
        is_second = lax.axis_index("stage") % 2
        low = jnp.where(is_second == 0, mine_all, twin_all)
        high = jnp.where(is_second == 0, twin_all, mine_all)
        return jnp.concatenate([low, high], axis=1)

    def layer(hidden, w_query, w_dkv, latent_gain, w_uk, w_uv, w_out):
        tokens = hidden[0]
        batch, seq_len, d_model = tokens.shape
        t_index = lax.axis_index("t")
        is_prompt = (lax.axis_index("stage") < half_stage).astype(jnp.int32)
        cos_tab, sin_tab = rope_tables(seq_len)
        cos4 = jnp.concatenate([cos_tab] * 4, axis=-1)
        sin4 = jnp.concatenate([-sin_tab, sin_tab, -sin_tab, sin_tab], axis=-1)

        n_away = batch // n_tp
        n_main = batch - 2 * n_away
        x_a = lax.ppermute(lax.dynamic_slice_in_dim(tokens, t_index * n_away, 1, axis=0), "stage", hand_pairs)
        x_b = lax.ppermute(lax.dynamic_slice_in_dim(tokens, t_index * n_away + 1, 1, axis=0), "stage", hand_pairs)

        n_heads = w_uk.shape[1] // NOPE_DIM
        by_head = w_query.reshape(d_model, n_heads, HEAD_DIM)
        wq_local = jnp.concatenate([by_head[:, :, :NOPE_DIM].reshape(d_model, -1), by_head[:, :, NOPE_DIM:].reshape(d_model, -1)], axis=1)
        wukv_local = jnp.concatenate([w_uk, w_uv], axis=1)
        wq_halves = gather_shards(wq_local)
        wukv_all = join_halves(*gather_shards(wukv_local))
        wo_halves = gather_shards(w_out)
        o_total = n_tp * n_heads * V_DIM

        odd = lax.rem(t_index, 2)
        neighbour = t_index + 1 - 2 * odd
        common = 2 * n_away * (1 - t_index // 2)
        order = jnp.stack([common + 2 + odd, common + odd, neighbour * n_away, neighbour * n_away + 1]).astype(jnp.int32)
        swapped_in = (common + 3 - odd, common + 1 - odd)
        wd = jnp.concatenate([w_dkv, jnp.zeros((d_model, 128 - ROPE_DIM), w_dkv.dtype)], axis=1)
        gain = latent_gain.astype(jnp.float32)[None]
        zero = jnp.zeros((1,), jnp.int32)
        prompt = is_prompt[None]
        here = t_index[None].astype(jnp.int32)
        away = lax.rem(t_index + 1 + jnp.arange(n_tp - 1, dtype=jnp.int32), n_tp)
        order_here = order * is_prompt
        cache_side = 1 - prompt
        second = lax.rem(lax.axis_index("stage"), 2)[None]
        tables = (cos4, sin4)

        def meta(*parts):
            return jnp.concatenate([p.astype(jnp.int32) for p in parts])

        def local_heads(active, xs, n_req, first, x, ckv, krp):
            return heads_call(meta(active, zero, zero, here, xs), 1, n_req, first, x, ckv, krp, wq_local[None], wq_local[None], 1, wukv_local[None], *tables, o_total, None)

        def rest_heads(active, xs, n_req, first, x, ckv, krp, o_mix):
            places = jnp.where(active == 1, away, away[:1])
            return heads_call(meta(active, second, places, places, xs), n_tp - 1, n_req, first, x, ckv, krp, *wq_halves, 0, wukv_all, *tables, o_total, o_mix)

        ckv, krp = latent_call(meta(prompt, order_here), n_main, tokens, wd, gain, *tables)
        o_swap = local_heads(prompt, order_here[:1], 1, 0, tokens, ckv, krp)
        o_swap2 = local_heads(prompt, order_here[1:2], 1, 1, tokens, ckv, krp)
        o_main = local_heads(prompt, order_here[2:], n_main - 2, 2, tokens, ckv, krp)

        def on_cache_side(x):
            ckv_s, krp_s = latent_call(meta(cache_side, zero), 1, x, wd, gain, *tables)
            o_s = local_heads(cache_side, zero, 1, 0, x, ckv_s, krp_s)
            o_s = rest_heads(cache_side, zero, 1, 0, x, ckv_s, krp_s, o_s)
            y_s = out_call(meta(cache_side, second, zero), 1, 0, o_s, *wo_halves, 1, False)
            back = lax.ppermute(y_s, "stage", back_pairs)
            return back, jnp.concatenate([ckv_s, krp_s[..., :ROPE_DIM]], axis=-1)

        back_a, latent_a = on_cache_side(x_a)

        def for_both(place, o_s):
            o_s = rest_heads(prompt, order_here[place : place + 1], 1, place, tokens, ckv, krp, o_s)
            y_s = out_call(meta(prompt, second, zero), 1, place, o_s, *wo_halves, 1, True)
            return y_s, lax.ppermute(y_s, "t", [(t, t ^ 1) for t in range(n_tp)])

        y_swap, from_swap = for_both(0, o_swap)
        y_swap2, from_swap2 = for_both(1, o_swap2)
        back_b, latent_b = on_cache_side(x_b)
        o_main = rest_heads(prompt, order_here[2:], n_main - 2, 2, tokens, ckv, krp, o_main)

        rows = out_call(meta(prompt, second, order[2:]), n_main - 2, 2, o_main, *wo_halves, batch, True)
        placed = ((y_swap, order[0]), (y_swap2, order[1]), (back_a, t_index * n_away), (from_swap, swapped_in[0]), (from_swap2, swapped_in[1]), (back_b, t_index * n_away + 1))
        for piece, place in placed:
            rows = lax.dynamic_update_slice_in_dim(rows, piece, place, axis=0)
        latent = jnp.concatenate([latent_a, latent_b], axis=0)
        latent = jnp.where(is_prompt == 1, jnp.zeros_like(latent), latent)
        return rows[None], latent[None]

    return jax.shard_map(layer, mesh=mesh, in_specs=(slot_spec, P(None, "t"), P(None, None), P(None), P(None, "t"), P(None, "t"), P("t", None)), out_specs=(slot_spec, cache_spec), check_vma=False)
```
